32 devices in a mesh: rep: 2 (over x), shard: 16 (over z, y, core).
Axes of the slice: x: 2, y: 2, z: 4, core: 2. Of those that a mesh axis runs over, the one named last changes fastest.
Arguments:
- tokens_x: bfloat16 [8192, 4096], P(('rep', 'shard')), may hold values from -6 to 6
- key_grad: bfloat16 [8192, 1024], P(('rep', 'shard')), may hold values from -0.06591797 to 0.06591797
- left_root: bfloat16 [64, 512, 512], P('shard'), may hold values from -1 to 3
- slot_grads: bfloat16 [64, 512, 512], P('shard'), may hold values from -6 to 6
- right_root: bfloat16 [64, 512, 512], P('shard'), may hold values from -1 to 3
- block_slot: int32 [32], replicated, may hold values from 0 to 63, as said below
Outputs:
- grad_key: float32 [4096, 1024], P('shard')
- update: bfloat16 [512, 32, 512], P('shard')
The draws below stay inside these ranges and needn't reach their ends.
Inputs may be any that keep to these rules, and one draw needn't show every extreme that they name: `block_slot`: the entries are distinct; slot v is slot v % 4 of shard index v // 4; no shard index holds more than 4 blocks, and some shard index holds exactly 4.
All inputs are finite; a program needn't handle non-finite values.
Results may differ from the reference program's by a relative error of at most 0.006.
Values may be sent and summed in bfloat16 or wider, within the bound.
No kernel may reach another device: no remote copies, remote signals or barrier semaphores. Data moves between devices by JAX's collectives and lax.ppermute only.
A program may use at most 128 MiB of HBM per device.

```python
import jax
import jax.numpy as jnp
from jax import lax

D = 4096
KEY_WIDTH = 1024
TOK_DEV = 256
BLOCK = 512
SLOTS = 4
NBLK = 32
SLOT_ALL = 64
TOKENS = 8192


def root_matrix(key):
    first_key, second_key = jax.random.split(key)
    diagonal = jnp.exp(jax.random.uniform(first_key, (SLOT_ALL, BLOCK), jnp.float32, jnp.log(0.5), jnp.log(2.0)))
    noise = jax.random.normal(second_key, (SLOT_ALL, BLOCK, BLOCK), jnp.float32)
    symmetric = (noise + jnp.swapaxes(noise, 1, 2)) * (0.5 / (2.0 * BLOCK) ** 0.5)
    symmetric = jnp.clip(symmetric, -0.9, 0.9)
    identity = jnp.eye(BLOCK, dtype=jnp.float32)
    return (symmetric + diagonal[:, :, None] * identity[None, :, :]).astype(jnp.bfloat16)


def draw_left_root(key, part):
    return root_matrix(jax.random.fold_in(key, 11))


def draw_right_root(key, part):
    return root_matrix(jax.random.fold_in(key, 23))


def draw_block_slot(key, part):
    base_key = jax.random.fold_in(key, 37)
    first_key, second_key, third_key = jax.random.split(base_key, 3)
    full_owner = jax.random.randint(first_key, (), 0, SLOT_ALL // SLOTS)
    slot_ids = jnp.arange(SLOT_ALL, dtype=jnp.int32)
    ranking = jax.random.permutation(second_key, SLOT_ALL).astype(jnp.int32)
    ranking = jnp.where(slot_ids // SLOTS == full_owner, slot_ids % SLOTS - SLOTS, ranking)
    chosen = jnp.argsort(ranking, stable=True)[:NBLK].astype(jnp.int32)
    shuffled = jax.random.permutation(third_key, NBLK).astype(jnp.int32)
    return chosen[shuffled].astype(jnp.int32)


def strengthened(array, rng, source, target, parts, factor):
    def block_of(position):
        return (jnp.arange(array.shape[position]) // (array.shape[position] // parts)).reshape((-1,) + (1,) * (array.ndim - 1 - position))

    near = jax.random.permutation(rng, parts)[block_of(target)]
    second = (block_of(target) + parts // 2) % parts
    return jnp.where((block_of(source) == near) | (block_of(source) == second), factor * array, array)


def block_levels(own_key, shape, cuts, least, top_value):
    gain, own = 1.0, jax.random.fold_in(own_key, 6)
    for axis_at, shards_of in cuts:
        draws = jnp.exp(jax.random.uniform(jax.random.fold_in(own, axis_at), (shards_of,), jnp.float32, least / len(cuts), top_value / len(cuts)))
        gain = gain * jnp.repeat(draws, shape[axis_at] // shards_of).reshape([-1 if axis == axis_at else 1 for axis in range(len(shape))])
    return gain


def normal_values(rng, dims, scale, reach, cuts=(), kind=jnp.bfloat16):
    entries = jax.random.normal(rng, dims, jnp.float32) * scale
    if len(cuts) > 0:
        entries = block_levels(rng, dims, cuts, -0.22, 0.18) * entries
    return jnp.clip(entries, min=-reach, max=reach).astype(kind)


def noise_with(stream_key, extent, spread, reach, cuts, heavy, kind=jnp.bfloat16):
    drawn = spread * jax.random.normal(stream_key, extent, jnp.float32)
    if cuts:
        drawn = drawn * block_levels(stream_key, extent, cuts, -0.22, 0.18)
    return jnp.clip(strengthened(drawn, jax.random.fold_in(stream_key, 3), *heavy), -reach, reach).astype(kind)


def setup_inputs(seed: int = 0) -> dict:
    keys = jax.random.split(jax.random.key(seed), 7)
    return {
        "tokens_x": noise_with(keys[0], (TOKENS, D), 1.0, 6.0, ((0, 32),), (0, 1, 32, 2.75)),
        "key_grad": normal_values(keys[1], (TOKENS, KEY_WIDTH), (TOKENS ** -0.5), 0.06591797, ((0, 32),)),
        "left_root": draw_left_root(jax.random.fold_in(keys[6], 71), 0),
        "slot_grads": normal_values(keys[3], (SLOT_ALL, BLOCK, BLOCK), 1.0, 6.0, ((0, 16),)),
        "right_root": draw_right_root(jax.random.fold_in(keys[6], 71), 0),
        "block_slot": draw_block_slot(jax.random.fold_in(keys[6], 71), 0),
    }


def reference(tokens_x, key_grad, left_root, slot_grads, right_root, block_slot):
    step_count = TOKENS // TOK_DEV
    token_blocks = tokens_x.reshape(step_count, TOK_DEV, D)
    grad_blocks = key_grad.reshape(step_count, TOK_DEV, KEY_WIDTH)

    def accumulate(total, pieces):
        rows_in, grads_in = pieces
        added = jnp.dot(rows_in.astype(jnp.float32).T, grads_in.astype(jnp.float32), preferred_element_type=jnp.float32)
        return total + added, None

    grad_key, ignored = lax.scan(accumulate, jnp.zeros((D, KEY_WIDTH), jnp.float32), (token_blocks, grad_blocks))

    def precondition(slot_index):
        left_part = jnp.dot(left_root[slot_index].astype(jnp.float32), slot_grads[slot_index].astype(jnp.float32), preferred_element_type=jnp.float32).astype(jnp.bfloat16)
        return jnp.dot(left_part.astype(jnp.float32), right_root[slot_index].astype(jnp.float32), preferred_element_type=jnp.float32).astype(jnp.bfloat16)

    blocks = lax.map(precondition, block_slot)
    update = jnp.transpose(blocks, (1, 0, 2))
    return grad_key, update
```

```python
import jax
import jax.numpy as jnp
from jax import lax
from jax.sharding import PartitionSpec as P

AXES = ("rep", "shard")
CHUNKS = 2


def rows_product(features, cotangent):
    return lax.dot_general(
        features, cotangent, (((0,), (0,)), ((), ())), preferred_element_type=jnp.float32
    )


def shards(tokens_x, key_grad, left_root, slot_grads, right_root, block_slot):
    n_rep, n_shard = lax.axis_size("rep"), lax.axis_size("shard")
    n_out = n_shard // 4
    x, s = lax.axis_index("rep"), lax.axis_index("shard")
    o, y, c = s // 4, s // 2 % 2, s % 2
    bf16, f32 = jnp.bfloat16, jnp.float32

    def permute(value, target):
        pairs = []
        for r in range(n_rep):
            for t in range(n_shard):
                r2, t2 = target(r, t)
                pairs.append((r * n_shard + t, r2 * n_shard + t2))
        return lax.ppermute(value, AXES, pairs)

    def swap_rep(value):
        return permute(value, lambda r, t: (1 - r, t))

    def swap_row(value):
        return permute(value, lambda r, t: (r, t ^ 2))

    def swap_core(value):
        return permute(value, lambda r, t: (r, t ^ 1))

    def shift_out(value, k):
        return permute(value, lambda r, t: (r, (t // 4 + k) % n_out * 4 + t % 4))

    def pick(value, index, axis):
        return lax.dynamic_index_in_dim(value, index, axis, keepdims=False)

    tok, width = key_grad.shape
    depth = tokens_x.shape[1]
    rows = depth // n_shard
    quarter = width // 4
    striped = tokens_x.reshape(tok, n_out * 2, 2, rows)
    mine = pick(striped, c, 2).reshape(tok, depth // 2)
    theirs = pick(striped, 1 - c, 2).reshape(tok, depth // 2)
    other_key = swap_core(key_grad)
    other_mine = swap_core(theirs)

    slots, order, _ = left_root.shape
    half = order // n_shard // 2
    own_rows = pick(left_root.reshape(slots, n_shard, 2, half, order), x, 2)
    own_rows = own_rows.reshape(slots, n_shard * half, order)
    left_part = jnp.einsum(
        "sij,sjk->sik", own_rows, slot_grads, preferred_element_type=f32
    ).astype(bf16)
    product = jnp.einsum(
        "sij,sjk->sik", left_part, right_root, preferred_element_type=f32
    ).astype(bf16)
    product = product.reshape(slots, n_out, 2, 2, half, order)
    by_out = [pick(product, o, 1)]
    for k in range(1, n_out):
        by_out.append(shift_out(pick(product, (o + k) % n_out, 1), k))
    by_out = jnp.stack(by_out)

    features = jnp.concatenate([mine, other_mine], 0)
    keys = jnp.concatenate([key_grad, other_key], 0)
    keys_a, keys_b = keys[:, : 2 * quarter], keys[:, 2 * quarter :]
    keys_a_own = lax.dynamic_slice_in_dim(keys_a, x * quarter, quarter, 1)
    keys_a_far = lax.dynamic_slice_in_dim(keys_a, (1 - x) * quarter, quarter, 1)
    chunks = min(CHUNKS, n_out)
    per = n_out // chunks
    total = None
    for j in range(chunks):
        shifts = [1 + j * per + m for m in range(per)]
        cols = [
            lax.dynamic_slice_in_dim(features, (o + k) % n_out * 2 * rows, 2 * rows, 1)
            for k in shifts
        ]
        both = jnp.concatenate(cols, 1) if per > 1 else cols[0]
        split = both.reshape(2 * tok, per, 2, rows)
        near = pick(split, y, 2).reshape(2 * tok, per * rows)
        far = pick(split, 1 - y, 2).reshape(2 * tok, per * rows)
        sent_a = rows_product(both, keys_a_far).astype(bf16)
        sent_b = rows_product(far, keys_b).astype(bf16)
        got_a = swap_rep(sent_a)
        got_b = swap_row(sent_b)
        sum_a = (rows_product(both, keys_a_own) + got_a.astype(f32)).reshape(
            per, 2, rows, quarter
        )
        sum_b = (rows_product(near, keys_b) + got_b.astype(f32)).reshape(
            per, rows, 2, quarter
        )
        got_a = swap_row(pick(sum_a, 1 - y, 1).astype(bf16))
        got_b = swap_rep(pick(sum_b, 1 - x, 2).astype(bf16))
        sum_a = pick(sum_a, y, 1) + got_a.astype(f32)
        sum_b = pick(sum_b, x, 2) + got_b.astype(f32)
        for m, k in enumerate(shifts):
            piece = jnp.concatenate([sum_a[m], sum_b[m]], 1)
            if k < n_out:
                piece = shift_out(piece.astype(bf16), k).astype(f32)
            total = piece if total is None else total + piece
    done = lax.reduce_precision(total, 8, 7)
    far_done = swap_rep(done.astype(bf16)).astype(f32)
    low = jnp.where(x == 0, done, far_done)
    high = jnp.where(x == 0, far_done, done)
    grad_key = jnp.concatenate(
        [low[:, :quarter], high[:, :quarter], low[:, quarter:], high[:, quarter:]], 1
    )

    by_row = jnp.stack(
        [pick(by_out, y, 2), swap_row(pick(by_out, 1 - y, 2))]
    )
    by_core = jnp.stack(
        [pick(by_row, c, 3), swap_core(pick(by_row, 1 - c, 3))]
    )
    held = by_core.reshape(n_shard * slots, half, order)
    ids = jnp.arange(n_shard * slots, dtype=jnp.int32)
    slot_at = ids % slots
    k_at = ids // slots % n_out
    y_at = ids // (slots * n_out) % 2
    c_at = ids // (slots * n_out * 2)
    source = (o - k_at + n_out) % n_out * 4 + jnp.bitwise_xor(y, y_at) * 2 + jnp.bitwise_xor(c, c_at)
    slot_id = source * slots + slot_at
    chosen = (block_slot[:, None] == slot_id[None, :]).astype(bf16)
    kept = jnp.einsum("bv,vhj->hbj", chosen, held, preferred_element_type=f32).astype(bf16)
    far_kept = swap_rep(kept)
    update = lax.dynamic_slice_in_dim(
        jnp.concatenate([kept, far_kept, kept], 0), x * half, 2 * half, 0
    )
    return (grad_key, update)


def solution(mesh):
    return jax.shard_map(
        shards,
        mesh=mesh,
        in_specs=(
            P(("rep", "shard"), None),
            P(("rep", "shard"), None),
            P("shard", None, None),
            P("shard", None, None),
            P("shard", None, None),
            P(),
        ),
        out_specs=(P("shard", None), P("shard", None, None)),
        check_vma=False,
    )
```

```python
import functools
import math

import jax
import jax.numpy as jnp
from jax import lax
from jax.experimental import pallas as pl
from jax.experimental.pallas import tpu as pltpu
from jax.sharding import PartitionSpec as P


AXES = ("rep", "shard")
WIDE = 5
BF16, F32 = jnp.bfloat16, jnp.float32


def pick(value, index, axis):
    return lax.dynamic_index_in_dim(value, index, axis, keepdims=False)


def blocks_kernel(at, left, grads, right, *refs):
    *outs, held = refs
    n_out = len(outs)
    pair, _, group, _, half, order = left.shape
    rows = [left[p].reshape(n_out * group * half, order) for p in range(pair)]
    part = [
        jnp.dot(rows[p], grads[p], preferred_element_type=F32).astype(BF16) for p in range(pair)
    ]
    for p in range(pair):
        held[p] = jnp.dot(part[p], right[p], preferred_element_type=F32).astype(BF16)
    for k, out in enumerate(outs):
        first = pl.multiple_of((at[1] + k) % n_out * (group * half), group * half)
        for p in range(pair):
            out[p] = held[p, pl.ds(first, group * half), :].reshape(group, half, order)


def owned_blocks(at, left_root, slot_grads, right_root, n_shard):
    slots, order, _ = left_root.shape
    n_out, half = n_shard // 4, order // n_shard // 2
    if half % 16:
        own = pick(left_root.reshape(slots, n_shard, 2, half, order), at[0], 2)
        own = own.reshape(slots, n_shard * half, order)
        part = jnp.einsum("sij,sjk->sik", own, slot_grads, preferred_element_type=F32)
        full = jnp.einsum(
            "sij,sjk->sik", part.astype(BF16), right_root, preferred_element_type=F32
        ).astype(BF16)
        full = full.reshape(slots, n_out, 4, half, order)
        return [pick(full, (at[1] + k) % n_out, 1) for k in range(n_out)]
    pair = 2 if slots % 2 == 0 else 1
    square = pl.BlockSpec((pair, order, order), lambda s, at: (s, 0, 0))
    out_shape = jax.ShapeDtypeStruct((slots, 4, half, order), BF16)
    return pl.pallas_call(
        blocks_kernel,
        grid_spec=pltpu.PrefetchScalarGridSpec(
            num_scalar_prefetch=1,
            grid=(slots // pair,),
            in_specs=[
                pl.BlockSpec(
                    (pair, n_out, 4, 1, half, order), lambda s, at: (s, 0, 0, at[0], 0, 0)
                ),
                square,
                square,
            ],
            out_specs=[pl.BlockSpec((pair, 4, half, order), lambda s, at: (s, 0, 0, 0))] * n_out,
            scratch_shapes=[pltpu.VMEM((pair, n_shard * half, order), BF16)],
        ),
        out_shape=[out_shape] * n_out,
        compiler_params=pltpu.CompilerParams(vmem_limit_bytes=57 * 2**20),
        cost_estimate=pl.CostEstimate(
            flops=2 * slots * order**3, bytes_accessed=7 * slots * order**2, transcendentals=0
        ),
    )(at, left_root.reshape(slots, n_out, 4, 2, half, order), slot_grads, right_root)


def groups_of(n_out):
    cut = n_out // 2 + 1
    groups = [range(1, cut), range(cut, n_out), range(n_out, n_out + 1)]
    return [group for group in groups if len(group)]


def local_kernel(kernel, in_specs, out_specs, out_shape, scalars=0, flops=0, grid=(1,), scratch=()):
    moved = sum(2 * math.prod(shape.shape) * shape.dtype.itemsize for shape in out_shape)
    return pl.pallas_call(
        kernel,
        grid_spec=pltpu.PrefetchScalarGridSpec(
            num_scalar_prefetch=scalars,
            grid=grid,
            in_specs=in_specs,
            out_specs=out_specs,
            scratch_shapes=scratch,
        ),
        out_shape=out_shape,
        compiler_params=pltpu.CompilerParams(vmem_limit_bytes=16 * 2**20),
        cost_estimate=pl.CostEstimate(flops=flops + moved, bytes_accessed=moved, transcendentals=0),
    )


def grads_kernel(sizes, at, mine, other, key, other_key, sent_a, own_a, sent_b, own_b):
    n_out, start, wide, thin = sizes
    count, rows = sent_a.shape[1], sent_a.shape[3]
    o, y, c = at[1], at[2], at[3]
    base = 2 * wide
    for m in range(count):
        for near in (1, 0):
            row_group = y if near else 1 - y
            first = ((o + start + m) % n_out * 4 + row_group * 2 + c) * rows
            cols = pl.ds(pl.multiple_of(first, 128), rows)
            tile, other_tile = mine[:, cols], other[:, cols]

            def product(begin, size):
                kept = slice(begin, begin + size)
                return jnp.dot(key[kept, :], tile, preferred_element_type=F32) + jnp.dot(
                    other_key[kept, :], other_tile, preferred_element_type=F32
                )

            sent_a[near, m] = product(0, wide).astype(BF16)
            own_a[near, m] = product(wide, wide)
            out_b = own_b if near else sent_b
            out_b[0, m] = product(base, thin).astype(out_b.dtype)
            out_b[1, m] = product(base + thin, thin).astype(out_b.dtype)


def partial_rows(at, mine, other, key, other_key, n_shard, group, wide, thin):
    width, tok = key.shape
    n_out, rows = n_shard // 4, mine.shape[1] // n_shard
    count = len(group)
    if rows % 128:
        o, y, c = at[1], at[2], at[3]

        def select(tokens):
            cols = pick(tokens.reshape(tok, n_out, 2, 2, rows), c, 3)
            cols = jnp.stack([pick(cols, 1 - y, 2), pick(cols, y, 2)], 1)
            cols = jnp.concatenate([cols, cols], 2)
            return lax.dynamic_slice_in_dim(cols, o + group[0], count, 2)

        cols = jnp.concatenate([select(mine), select(other)], 0)
        keys = jnp.concatenate([key, other_key], 1)
        full = jnp.einsum("wt,tnkr->nkwr", keys, cols, preferred_element_type=F32)
        base = 2 * wide
        own_a, sent_a = full[:, :, wide:base], full[:, :, :wide]
        own_b = jnp.stack([full[1, :, base : base + thin], full[1, :, base + thin :]])
        sent_b = jnp.stack([full[0, :, base : base + thin], full[0, :, base + thin :]])
        return sent_a.astype(BF16), own_a, sent_b.astype(BF16), own_b
    vmem = pl.BlockSpec(memory_space=pltpu.VMEM)
    shape_a, shape_b = (2, count, wide, rows), (2, count, thin, rows)
    return local_kernel(
        functools.partial(grads_kernel, (n_out, group[0], wide, thin)),
        [vmem] * 4,
        [vmem] * 4,
        [
            jax.ShapeDtypeStruct(shape_a, BF16),
            jax.ShapeDtypeStruct(shape_a, F32),
            jax.ShapeDtypeStruct(shape_b, BF16),
            jax.ShapeDtypeStruct(shape_b, F32),
        ],
        scalars=1,
        flops=8 * tok * count * rows * width,
        grid=(),
    )(at, mine, other, key, other_key)


def fold_kernel(own, got, out):
    out[...] = (own[0] + got[0].astype(F32)).astype(BF16)


def folded(own, got):
    if own.shape[-1] % 128:
        return (own[0] + got[0].astype(F32)).astype(BF16)
    block = pl.BlockSpec((1,) + own.shape[1:], lambda i: (0, 0, 0, 0))
    return local_kernel(
        fold_kernel,
        [block, block],
        [pl.BlockSpec(own.shape[1:], lambda i: (0, 0, 0))],
        [jax.ShapeDtypeStruct(own.shape[1:], BF16)],
    )(own, got)[0]


def merge_kernel(own_a, got_a, last_a, own_b, got_b, last_b, *outs):
    wide = own_a.shape[2]
    for m, out in enumerate(outs):
        for part, own, got, last in (
            (slice(0, wide), own_a, got_a, last_a),
            (slice(wide, None), own_b, got_b, last_b),
        ):
            total = own[0, m] + got[0, m].astype(F32) + last[m].astype(F32)
            out[part, :] = total.astype(out.dtype)


def merged(own_a, got_a, last_a, own_b, got_b, last_b, types):
    count, wide, rows = own_a.shape[1:]
    thin = own_b.shape[2]
    if rows % 128:
        sum_a = own_a[1] + got_a[1].astype(F32) + last_a.astype(F32)
        sum_b = own_b[1] + got_b[1].astype(F32) + last_b.astype(F32)
        both = jnp.concatenate([sum_a, sum_b], 1)
        return [both[m].astype(dtype) for m, dtype in enumerate(types)]

    def specs(size):
        half = pl.BlockSpec((1, count, size, rows), lambda i: (1, 0, 0, 0))
        return [half, half, pl.BlockSpec((count, size, rows), lambda i: (0, 0, 0))]

    return local_kernel(
        merge_kernel,
        specs(wide) + specs(thin),
        [pl.BlockSpec((wide + thin, rows), lambda i: (0, 0))] * count,
        [jax.ShapeDtypeStruct((wide + thin, rows), dtype) for dtype in types],
    )(own_a, got_a, last_a, own_b, got_b, last_b)


def gather_kernel(at, *refs):
    *parts, out = refs
    for k, part in enumerate(parts):
        out[k] = part[...]


def row_sends(at, pieces):
    slots, _, half, order = pieces[0].shape
    if half % 16:
        return jnp.stack([lax.dynamic_slice_in_dim(p, (1 - at[2]) * 2, 2, 1) for p in pieces])
    part = (slots, 2, half, order)
    shape = (len(pieces),) + part
    return local_kernel(
        gather_kernel,
        [pl.BlockSpec(part, lambda i, at: (0, 1 - at[2], 0, 0))] * len(pieces),
        [pl.BlockSpec(shape, lambda i, at: (0, 0, 0, 0, 0))],
        [jax.ShapeDtypeStruct(shape, BF16)],
        scalars=1,
    )(at, *pieces)[0]


def core_kernel(at, *refs):
    *parts, row, near, far = refs
    c = at[3]
    for k, part in enumerate(parts):
        near[0, k], far[0, k] = part[:, c], part[:, 1 - c]
    near[1], far[1] = row[:, :, c], row[:, :, 1 - c]


def core_split(at, pieces, row):
    slots, _, half, order = pieces[0].shape
    n_out = len(pieces)
    if half % 16:
        own = jnp.stack([lax.dynamic_slice_in_dim(p, at[2] * 2, 2, 1) for p in pieces])
        both = jnp.stack([own, row])
        return pick(both, at[3], 3), pick(both, 1 - at[3], 3)
    shape = (2, n_out, slots, half, order)
    out = pl.BlockSpec(shape, lambda i, at: (0, 0, 0, 0, 0))
    return local_kernel(
        core_kernel,
        [pl.BlockSpec((slots, 2, half, order), lambda i, at: (0, at[2], 0, 0))] * n_out
        + [pl.BlockSpec(row.shape, lambda i, at: (0, 0, 0, 0, 0))],
        [out, out],
        [jax.ShapeDtypeStruct(shape, BF16)] * 2,
        scalars=1,
    )(at, *pieces, row)


def shards(tokens_x, key_grad, left_root, slot_grads, right_root, block_slot):
    n_rep, n_shard = lax.axis_size("rep"), lax.axis_size("shard")
    n_out = n_shard // 4
    x, s = lax.axis_index("rep"), lax.axis_index("shard")
    o, y, c = s // 4, s // 2 % 2, s % 2
    at = jnp.stack([x, o, y, c]).astype(jnp.int32)

    def permute(value, target):
        pairs = []
        for r in range(n_rep):
            for t in range(n_shard):
                r2, t2 = target(r, t)
                pairs.append((r * n_shard + t, r2 * n_shard + t2))
        return lax.ppermute(value, AXES, pairs)

    def swap_rep(value):
        return permute(value, lambda r, t: (1 - r, t))

    def swap_row(value):
        return permute(value, lambda r, t: (r, t ^ 2))

    def swap_core(value):
        return permute(value, lambda r, t: (r, t ^ 1))

    def shift_out(value, k):
        return permute(value, lambda r, t: (r, (t // 4 + k) % n_out * 4 + t % 4))

    width = key_grad.shape[1]
    wide = width * WIDE // 16
    thin = width // 2 - wide
    other_tokens = swap_core(tokens_x)
    key = key_grad.T
    low_a, high_a = key[:wide], key[wide : 2 * wide]
    low_b, high_b = key[2 * wide : 2 * wide + thin], key[2 * wide + thin :]
    key = jnp.where(
        x == 0,
        jnp.concatenate([high_a, low_a, high_b, low_b], 0),
        jnp.concatenate([low_a, high_a, low_b, high_b], 0),
    )
    other_key = swap_core(key)

    slots, order, _ = left_root.shape
    half = order // n_shard // 2
    pieces = owned_blocks(at, left_root, slot_grads, right_root, n_shard)
    by_out = [pieces[0]] + [shift_out(pieces[k], k) for k in range(1, n_out)]

    finished = []
    for group in groups_of(n_out):
        sent_a, own_a, sent_b, own_b = partial_rows(
            at, tokens_x, other_tokens, key, other_key, n_shard, group, wide, thin
        )
        got_a = swap_rep(sent_a)
        got_b = swap_row(sent_b)
        far_a = folded(own_a, got_a)
        far_b = folded(own_b, got_b)
        last_a = swap_row(far_a)
        last_b = swap_rep(far_b)
        sums = merged(
            own_a, got_a, last_a, own_b, got_b, last_b,
            [BF16 if k < n_out else F32 for k in group],
        )
        for k, piece in zip(group, sums):
            finished.append(shift_out(piece, k) if k < n_out else piece)

    sent_row = row_sends(at, by_out)
    got_row = swap_row(sent_row)
    near_core, far_core = core_split(at, by_out, got_row)
    held = jnp.stack([near_core, swap_core(far_core)])
    held = held.reshape(n_shard * slots, half, order)
    ids = jnp.arange(n_shard * slots, dtype=jnp.int32)
    source_out = (o - ids // slots % n_out + n_out) % n_out
    source_row = jnp.bitwise_xor(y, ids // (slots * n_out) % 2)
    source_core = jnp.bitwise_xor(c, ids // (slots * n_out * 2))
    slot_id = (source_out * 4 + source_row * 2 + source_core) * slots + ids % slots
    chosen = (block_slot[:, None] == slot_id[None, :]).astype(BF16)
    kept = jnp.einsum("bv,vhj->hbj", chosen, held, preferred_element_type=F32).astype(BF16)
    total = finished[-1]
    for piece in finished[:-1]:
        total = total + piece.astype(F32)
    done = lax.reduce_precision(total, 8, 7)
    far_done = swap_rep(done.astype(BF16)).astype(F32)
    low = jnp.where(x == 0, done, far_done)
    high = jnp.where(x == 0, far_done, done)
    grad_key = jnp.concatenate([low[:wide], high[:wide], low[wide:], high[wide:]], 0).T

    far_kept = swap_rep(kept)
    update = lax.dynamic_slice_in_dim(
        jnp.concatenate([kept, far_kept, kept], 0), x * half, 2 * half, 0
    )
    return (grad_key, update)


def solution(mesh):
    return jax.shard_map(
        shards,
        mesh=mesh,
        in_specs=(
            P(("rep", "shard"), None),
            P(("rep", "shard"), None),
            P("shard", None, None),
            P("shard", None, None),
            P("shard", None, None),
            P(),
        ),
        out_specs=(P("shard", None), P("shard", None, None)),
        check_vma=False,
    )
```

```python
import functools
import math

import jax
import jax.numpy as jnp
from jax import lax
from jax.experimental import pallas as pl
from jax.experimental.pallas import tpu as pltpu
from jax.sharding import PartitionSpec as P


AXES = ("rep", "shard")
WIDE = 5
BF16, F32 = jnp.bfloat16, jnp.float32


def pick(value, index, axis):
    return lax.dynamic_index_in_dim(value, index, axis, keepdims=False)


def blocks_kernel(at, left, grads, right, *refs):
    *outs, held = refs
    n_out = len(outs)
    pair, _, group, _, half, order = left.shape
    rows = [left[p].reshape(n_out * group * half, order) for p in range(pair)]
    part = [
        jnp.dot(rows[p], grads[p], preferred_element_type=F32).astype(BF16) for p in range(pair)
    ]
    for p in range(pair):
        held[p] = jnp.dot(part[p], right[p], preferred_element_type=F32).astype(BF16)
    for k, out in enumerate(outs):
        first = pl.multiple_of((at[1] + k) % n_out * (group * half), group * half)
        for p in range(pair):
            out[p] = held[p, pl.ds(first, group * half), :].reshape(group, half, order)


def owned_blocks(at, left_root, slot_grads, right_root, n_shard):
    slots, order, _ = left_root.shape
    n_out, half = n_shard // 4, order // n_shard // 2
    if half % 16:
        own = pick(left_root.reshape(slots, n_shard, 2, half, order), at[0], 2)
        own = own.reshape(slots, n_shard * half, order)
        part = jnp.einsum("sij,sjk->sik", own, slot_grads, preferred_element_type=F32)
        full = jnp.einsum(
            "sij,sjk->sik", part.astype(BF16), right_root, preferred_element_type=F32
        ).astype(BF16)
        full = full.reshape(slots, n_out, 4, half, order)
        return [pick(full, (at[1] + k) % n_out, 1) for k in range(n_out)]
    pair = 2 if slots % 2 == 0 else 1
    square = pl.BlockSpec((pair, order, order), lambda s, at: (s, 0, 0))
    out_shape = jax.ShapeDtypeStruct((slots, 4, half, order), BF16)
    return pl.pallas_call(
        blocks_kernel,
        grid_spec=pltpu.PrefetchScalarGridSpec(
            num_scalar_prefetch=1,
            grid=(slots // pair,),
            in_specs=[
                pl.BlockSpec(
                    (pair, n_out, 4, 1, half, order), lambda s, at: (s, 0, 0, at[0], 0, 0)
                ),
                square,
                square,
            ],
            out_specs=[pl.BlockSpec((pair, 4, half, order), lambda s, at: (s, 0, 0, 0))] * n_out,
            scratch_shapes=[pltpu.VMEM((pair, n_shard * half, order), BF16)],
        ),
        out_shape=[out_shape] * n_out,
        compiler_params=pltpu.CompilerParams(vmem_limit_bytes=57 * 2**20),
        cost_estimate=pl.CostEstimate(
            flops=2 * slots * order**3, bytes_accessed=7 * slots * order**2, transcendentals=0
        ),
    )(at, left_root.reshape(slots, n_out, 4, 2, half, order), slot_grads, right_root)


def groups_of(n_out):
    cut = n_out // 2 + 1
    groups = [range(1, cut), range(cut, n_out), range(n_out, n_out + 1)]
    return [group for group in groups if len(group)]


def local_kernel(kernel, in_specs, out_specs, out_shape, scalars=0, flops=0, grid=(1,), scratch=()):
    moved = sum(2 * math.prod(shape.shape) * shape.dtype.itemsize for shape in out_shape)
    return pl.pallas_call(
        kernel,
        grid_spec=pltpu.PrefetchScalarGridSpec(
            num_scalar_prefetch=scalars,
            grid=grid,
            in_specs=in_specs,
            out_specs=out_specs,
            scratch_shapes=scratch,
        ),
        out_shape=out_shape,
        compiler_params=pltpu.CompilerParams(vmem_limit_bytes=16 * 2**20),
        cost_estimate=pl.CostEstimate(flops=flops + moved, bytes_accessed=moved, transcendentals=0),
    )


def grads_kernel(sizes, at, mine, other, key, other_key, *outs):
    n_out, start, wide, thin = sizes
    sent_a, own_a, *outs_b = outs
    count, rows = sent_a.shape[1], sent_a.shape[3]
    o, y, c = at[1], at[2], at[3]
    base = 2 * wide
    for m in range(count):
        for near in (1, 0):
            row_group = y if near else 1 - y
            first = ((o + start + m) % n_out * 4 + row_group * 2 + c) * rows
            cols = pl.ds(pl.multiple_of(first, 128), rows)
            tile, other_tile = mine[:, cols], other[:, cols]

            def product(begin, size):
                kept = slice(begin, begin + size)
                return jnp.dot(key[kept, :], tile, preferred_element_type=F32) + jnp.dot(
                    other_key[kept, :], other_tile, preferred_element_type=F32
                )

            sent_a[near, m, :wide] = product(0, wide).astype(BF16)
            own_a[near, m, :wide] = product(wide, wide)
            far, close = product(base, thin), product(base + thin, thin)
            if outs_b:
                out_b = outs_b[near]
                out_b[0, m] = far.astype(out_b.dtype)
                out_b[1, m] = close.astype(out_b.dtype)
            else:
                sent_a[near, m, wide:] = far.astype(BF16)
                own_a[near, m, wide:] = close


def partial_rows(at, mine, other, key, other_key, n_shard, group, wide, thin, split):
    width, tok = key.shape
    n_out, rows = n_shard // 4, mine.shape[1] // n_shard
    count = len(group)
    if rows % 128:
        o, y, c = at[1], at[2], at[3]

        def select(tokens):
            cols = pick(tokens.reshape(tok, n_out, 2, 2, rows), c, 3)
            cols = jnp.stack([pick(cols, 1 - y, 2), pick(cols, y, 2)], 1)
            cols = jnp.concatenate([cols, cols], 2)
            return lax.dynamic_slice_in_dim(cols, o + group[0], count, 2)

        cols = jnp.concatenate([select(mine), select(other)], 0)
        keys = jnp.concatenate([key, other_key], 1)
        full = jnp.einsum("wt,tnkr->nkwr", keys, cols, preferred_element_type=F32)
        base = 2 * wide
        far_b, near_b = full[:, :, base : base + thin], full[:, :, base + thin :]
        sent_a, own_a = full[:, :, :wide], full[:, :, wide:base]
        if not split:
            sent_a = jnp.concatenate([sent_a, far_b], 2)
            return sent_a.astype(BF16), jnp.concatenate([own_a, near_b], 2)
        sent_b, own_b = (jnp.stack([far_b[n], near_b[n]]) for n in (0, 1))
        return sent_a.astype(BF16), own_a, sent_b.astype(BF16), own_b
    vmem = pl.BlockSpec(memory_space=pltpu.VMEM)
    heights = (wide, thin) if split else (wide + thin,)
    return local_kernel(
        functools.partial(grads_kernel, (n_out, group[0], wide, thin)),
        [vmem] * 4,
        [vmem] * (2 * len(heights)),
        [
            jax.ShapeDtypeStruct((2, count, height, rows), dtype)
            for height in heights
            for dtype in (BF16, F32)
        ],
        scalars=1,
        flops=8 * tok * count * rows * width,
        grid=(),
    )(at, mine, other, key, other_key)


def fold_kernel(own, got, out):
    out[...] = (own[0] + got[0].astype(F32)).astype(BF16)


def folded(own, got):
    if own.shape[-1] % 128:
        return (own[0] + got[0].astype(F32)).astype(BF16)
    block = pl.BlockSpec((1,) + own.shape[1:], lambda i: (0, 0, 0, 0))
    return local_kernel(
        fold_kernel,
        [block, block],
        [pl.BlockSpec(own.shape[1:], lambda i: (0, 0, 0))],
        [jax.ShapeDtypeStruct(own.shape[1:], BF16)],
    )(own, got)[0]


def merge_kernel(heights, *refs):
    first = 0
    for i, height in enumerate(heights):
        own, got, last = refs[3 * i : 3 * i + 3]
        for m, out in enumerate(refs[3 * len(heights) :]):
            total = own[0, m] + got[0, m].astype(F32) + last[m].astype(F32)
            out[first : first + height, :] = total.astype(out.dtype)
        first += height


def merged(parts, types):
    count, rows = len(types), parts[0][0].shape[3]
    heights = [own.shape[2] for own, _, _ in parts]
    if rows % 128:
        sums = [own[1] + got[1].astype(F32) + last.astype(F32) for own, got, last in parts]
        both = jnp.concatenate(sums, 1)
        return [both[m].astype(dtype) for m, dtype in enumerate(types)]
    in_specs = []
    for height in heights:
        half = pl.BlockSpec((1, count, height, rows), lambda i: (1, 0, 0, 0))
        in_specs += [half, half, pl.BlockSpec((count, height, rows), lambda i: (0, 0, 0))]
    shape = (sum(heights), rows)
    return local_kernel(
        functools.partial(merge_kernel, heights),
        in_specs,
        [pl.BlockSpec(shape, lambda i: (0, 0))] * count,
        [jax.ShapeDtypeStruct(shape, dtype) for dtype in types],
    )(*(value for part in parts for value in part))


def spread_kernel(at, *refs):
    outs = refs[-4:]
    y, c = at[2], at[3]
    places = [row * 2 + core for core in (c, 1 - c) for row in (y, 1 - y)]
    for k, piece in enumerate(refs[:-4]):
        for place, out in zip(places, outs):
            out[k] = piece[:, place]


def spread(at, pieces):
    slots, _, half, order = pieces[0].shape
    shape = (len(pieces), slots, half, order)
    if half % 16:
        both = jnp.stack(pieces)
        places = [row * 2 + core for core in (at[3], 1 - at[3]) for row in (at[2], 1 - at[2])]
        return [pick(both, place, 2) for place in places]
    whole = pl.BlockSpec(pieces[0].shape, lambda i, at: (0, 0, 0, 0))
    return local_kernel(
        spread_kernel,
        [whole] * len(pieces),
        [pl.BlockSpec(shape, lambda i, at: (0, 0, 0, 0))] * 4,
        [jax.ShapeDtypeStruct(shape, BF16)] * 4,
        scalars=1,
    )(at, *pieces)


def shards(tokens_x, key_grad, left_root, slot_grads, right_root, block_slot):
    n_rep, n_shard = lax.axis_size("rep"), lax.axis_size("shard")
    n_out = n_shard // 4
    x, s = lax.axis_index("rep"), lax.axis_index("shard")
    o, y, c = s // 4, s // 2 % 2, s % 2
    at = jnp.stack([x, o, y, c]).astype(jnp.int32)

    def permute(value, target):
        pairs = []
        for r in range(n_rep):
            for t in range(n_shard):
                r2, t2 = target(r, t)
                pairs.append((r * n_shard + t, r2 * n_shard + t2))
        return lax.ppermute(value, AXES, pairs)

    def swap_rep(value):
        return permute(value, lambda r, t: (1 - r, t))

    def swap_row(value):
        return permute(value, lambda r, t: (r, t ^ 2))

    def swap_core(value):
        return permute(value, lambda r, t: (r, t ^ 1))

    def shift_out(value, k):
        return permute(value, lambda r, t: (r, (t // 4 + k) % n_out * 4 + t % 4))

    width = key_grad.shape[1]
    wide = width * WIDE // 16
    thin = width // 2 - wide
    other_tokens = swap_core(tokens_x)
    key = key_grad.T
    low_a, high_a = key[:wide], key[wide : 2 * wide]
    low_b, high_b = key[2 * wide : 2 * wide + thin], key[2 * wide + thin :]
    key = jnp.where(
        x == 0,
        jnp.concatenate([high_a, low_a, high_b, low_b], 0),
        jnp.concatenate([low_a, high_a, low_b, high_b], 0),
    )
    other_key = swap_core(key)

    slots, order, _ = left_root.shape
    half = order // n_shard // 2
    pieces = owned_blocks(at, left_root, slot_grads, right_root, n_shard)
    by_out = [pieces[0]] + [shift_out(pieces[k], k) for k in range(1, n_out)]

    finished = []
    for group in groups_of(n_out):
        kept = partial_rows(
            at, tokens_x, other_tokens, key, other_key, n_shard, group, wide, thin,
            group[-1] < n_out,
        )
        got_a = swap_rep(kept[0])
        far_a = folded(kept[1], got_a)
        parts = [(kept[1], got_a, swap_row(far_a))]
        if len(kept) > 2:
            got_b = swap_row(kept[2])
            far_b = folded(kept[3], got_b)
            parts.append((kept[3], got_b, swap_rep(far_b)))
        sums = merged(parts, [BF16 if k < n_out else F32 for k in group])
        for k, piece in zip(group, sums):
            finished.append(shift_out(piece, k) if k < n_out else piece)

    own, far_row, far_core, far_both = spread(at, by_out)
    far_row = swap_row(far_row)
    far_core = swap_core(far_core)
    far_both = permute(far_both, lambda r, t: (r, t ^ 3))
    held = jnp.stack([own, far_row, far_core, far_both])
    held = held.reshape(n_shard * slots, half, order)
    ids = jnp.arange(n_shard * slots, dtype=jnp.int32)
    source_out = (o - ids // slots % n_out + n_out) % n_out
    source_row = jnp.bitwise_xor(y, ids // (slots * n_out) % 2)
    source_core = jnp.bitwise_xor(c, ids // (slots * n_out * 2))
    slot_id = (source_out * 4 + source_row * 2 + source_core) * slots + ids % slots
    chosen = (block_slot[:, None] == slot_id[None, :]).astype(BF16)
    kept = jnp.einsum("bv,vhj->hbj", chosen, held, preferred_element_type=F32).astype(BF16)
    total = finished[-1]
    for piece in finished[:-1]:
        total = total + piece.astype(F32)
    done = lax.reduce_precision(total, 8, 7)
    far_done = swap_rep(done.astype(BF16)).astype(F32)
    low = jnp.where(x == 0, done, far_done)
    high = jnp.where(x == 0, far_done, done)
    grad_key = jnp.concatenate([low[:wide], high[:wide], low[wide:], high[wide:]], 0).T

    far_kept = swap_rep(kept)
    update = lax.dynamic_slice_in_dim(
        jnp.concatenate([kept, far_kept, kept], 0), x * half, 2 * half, 0
    )
    return (grad_key, update)


def solution(mesh):
    return jax.shard_map(
        shards,
        mesh=mesh,
        in_specs=(
            P(("rep", "shard"), None),
            P(("rep", "shard"), None),
            P("shard", None, None),
            P("shard", None, None),
            P("shard", None, None),
            P(),
        ),
        out_specs=(P("shard", None), P("shard", None, None)),
        check_vma=False,
    )
```

```python
import functools
import math

import jax
import jax.numpy as jnp
from jax import lax
from jax.experimental import pallas as pl
from jax.experimental.pallas import tpu as pltpu
from jax.sharding import PartitionSpec as P


AXES = ("rep", "shard")
WIDE = 5
BF16, F32 = jnp.bfloat16, jnp.float32


def position():
    s = lax.axis_index("shard")
    return lax.axis_index("rep"), s // 4, s // 2 % 2, s % 2


def pick(value, index, axis):
    return lax.dynamic_index_in_dim(value, index, axis, keepdims=False)


def blocks_kernel(wide, left, grads, right, key, *refs):
    *outs, key_out, held = refs
    n_out = len(outs)
    pair, _, group, _, half, order = left.shape
    x, o, _, _ = position()
    thin = key.shape[1] // 2 - wide

    @pl.when(pl.program_id(0) == 0)
    def _():
        turned = key[...].T
        for part, size, base in ((0, wide, 0), (2 * wide, thin, 2 * wide)):
            for i, first in ((0, (1 - x) * size), (1, x * size)):
                to = pl.ds(pl.multiple_of(base + first, 16), size)
                key_out[to, :] = turned[part + i * size : part + (i + 1) * size]

    rows = [left[p].reshape(n_out * group * half, order) for p in range(pair)]
    part = [
        jnp.dot(rows[p], grads[p], preferred_element_type=F32).astype(BF16) for p in range(pair)
    ]
    for p in range(pair):
        held[p] = jnp.dot(part[p], right[p], preferred_element_type=F32).astype(BF16)
    for k, out in enumerate(outs):
        first = pl.multiple_of((o + k) % n_out * (group * half), group * half)
        for p in range(pair):
            out[p] = held[p, pl.ds(first, group * half), :].reshape(group, half, order)


def owned_blocks(left_root, slot_grads, right_root, key, n_shard, wide):
    x, o, _, _ = position()
    slots, order, _ = left_root.shape
    n_out, half = n_shard // 4, order // n_shard // 2
    if half % 16:
        own = pick(left_root.reshape(slots, n_shard, 2, half, order), x, 2)
        own = own.reshape(slots, n_shard * half, order)
        part = jnp.einsum("sij,sjk->sik", own, slot_grads, preferred_element_type=F32)
        full = jnp.einsum(
            "sij,sjk->sik", part.astype(BF16), right_root, preferred_element_type=F32
        ).astype(BF16)
        full = full.reshape(slots, n_out, 4, half, order)
        turned = key.T
        base, thin = 2 * wide, key.shape[1] // 2 - wide
        low_a, high_a = turned[:wide], turned[wide:base]
        low_b, high_b = turned[base : base + thin], turned[base + thin :]
        turned = jnp.where(
            x == 0,
            jnp.concatenate([high_a, low_a, high_b, low_b], 0),
            jnp.concatenate([low_a, high_a, low_b, high_b], 0),
        )
        return [pick(full, (o + k) % n_out, 1) for k in range(n_out)], turned
    pair = 2 if slots % 2 == 0 else 1
    square = pl.BlockSpec((pair, order, order), lambda s: (s, 0, 0))
    out_shape = jax.ShapeDtypeStruct((slots, 4, half, order), BF16)
    turned = key.shape[::-1]
    *pieces, key = pl.pallas_call(
        functools.partial(blocks_kernel, wide),
        grid=(slots // pair,),
        in_specs=[
            pl.BlockSpec(
                (pair, n_out, 4, 1, half, order),
                lambda s: (s, 0, 0, lax.axis_index("rep"), 0, 0),
            ),
            square,
            square,
            pl.BlockSpec(key.shape, lambda s: (0, 0)),
        ],
        out_specs=[pl.BlockSpec((pair, 4, half, order), lambda s: (s, 0, 0, 0))] * n_out
        + [pl.BlockSpec(turned, lambda s: (0, 0))],
        scratch_shapes=[pltpu.VMEM((pair, n_shard * half, order), BF16)],
        out_shape=[out_shape] * n_out + [jax.ShapeDtypeStruct(turned, BF16)],
        compiler_params=pltpu.CompilerParams(vmem_limit_bytes=57 * 2**20),
        cost_estimate=pl.CostEstimate(
            flops=2 * slots * order**3, bytes_accessed=7 * slots * order**2, transcendentals=0
        ),
    )(left_root.reshape(slots, n_out, 4, 2, half, order), slot_grads, right_root, key)
    return pieces, key


def groups_of(n_out):
    cut = n_out // 2 + 1
    groups = [range(1, cut), range(cut, n_out), range(n_out, n_out + 1)]
    return [group for group in groups if len(group)]


def local_kernel(kernel, in_specs, out_specs, out_shape, flops=0, grid=(1,)):
    moved = sum(2 * math.prod(shape.shape) * shape.dtype.itemsize for shape in out_shape)
    return pl.pallas_call(
        kernel,
        grid=grid,
        in_specs=in_specs,
        out_specs=out_specs,
        out_shape=out_shape,
        compiler_params=pltpu.CompilerParams(vmem_limit_bytes=16 * 2**20),
        cost_estimate=pl.CostEstimate(flops=flops + moved, bytes_accessed=moved, transcendentals=0),
    )


def grads_kernel(sizes, mine, other, key, other_key, *outs):
    n_out, start, wide, thin = sizes
    sent_a, own_a, *outs_b = outs
    count, rows = sent_a.shape[1], sent_a.shape[3]
    _, o, y, c = position()
    base = 2 * wide
    for m in range(count):
        for near in (1, 0):
            row_group = y if near else 1 - y
            first = ((o + start + m) % n_out * 4 + row_group * 2 + c) * rows
            cols = pl.ds(pl.multiple_of(first, 128), rows)
            tile, other_tile = mine[:, cols], other[:, cols]

            def product(begin, size):
                kept = slice(begin, begin + size)
                return jnp.dot(key[kept, :], tile, preferred_element_type=F32) + jnp.dot(
                    other_key[kept, :], other_tile, preferred_element_type=F32
                )

            sent_a[near, m, :wide] = product(0, wide).astype(BF16)
            own_a[near, m, :wide] = product(wide, wide)
            far, close = product(base, thin), product(base + thin, thin)
            if outs_b:
                out_b = outs_b[near]
                out_b[0, m] = far.astype(out_b.dtype)
                out_b[1, m] = close.astype(out_b.dtype)
            else:
                sent_a[near, m, wide:] = far.astype(BF16)
                own_a[near, m, wide:] = close


def partial_rows(mine, other, key, other_key, n_shard, group, wide, thin, split):
    width, tok = key.shape
    n_out, rows = n_shard // 4, mine.shape[1] // n_shard
    count = len(group)
    if rows % 128:
        _, o, y, c = position()

        def select(tokens):
            cols = pick(tokens.reshape(tok, n_out, 2, 2, rows), c, 3)
            cols = jnp.stack([pick(cols, 1 - y, 2), pick(cols, y, 2)], 1)
            cols = jnp.concatenate([cols, cols], 2)
            return lax.dynamic_slice_in_dim(cols, o + group[0], count, 2)

        cols = jnp.concatenate([select(mine), select(other)], 0)
        keys = jnp.concatenate([key, other_key], 1)
        full = jnp.einsum("wt,tnkr->nkwr", keys, cols, preferred_element_type=F32)
        base = 2 * wide
        far_b, near_b = full[:, :, base : base + thin], full[:, :, base + thin :]
        sent_a, own_a = full[:, :, :wide], full[:, :, wide:base]
        if not split:
            sent_a = jnp.concatenate([sent_a, far_b], 2)
            return sent_a.astype(BF16), jnp.concatenate([own_a, near_b], 2)
        sent_b, own_b = (jnp.stack([far_b[n], near_b[n]]) for n in (0, 1))
        return sent_a.astype(BF16), own_a, sent_b.astype(BF16), own_b
    vmem = pl.BlockSpec(memory_space=pltpu.VMEM)
    heights = (wide, thin) if split else (wide + thin,)
    return local_kernel(
        functools.partial(grads_kernel, (n_out, group[0], wide, thin)),
        [vmem] * 4,
        [vmem] * (2 * len(heights)),
        [
            jax.ShapeDtypeStruct((2, count, height, rows), dtype)
            for height in heights
            for dtype in (BF16, F32)
        ],
        flops=8 * tok * count * rows * width,
        grid=(),
    )(mine, other, key, other_key)


def fold_kernel(own, got, out):
    out[...] = (own[0] + got[0].astype(F32)).astype(BF16)


def folded(own, got):
    if own.shape[-1] % 128:
        return (own[0] + got[0].astype(F32)).astype(BF16)
    block = pl.BlockSpec((1,) + own.shape[1:], lambda i: (0, 0, 0, 0))
    return local_kernel(
        fold_kernel,
        [block, block],
        [pl.BlockSpec(own.shape[1:], lambda i: (0, 0, 0))],
        [jax.ShapeDtypeStruct(own.shape[1:], BF16)],
    )(own, got)[0]


def merge_kernel(heights, *refs):
    first = 0
    for i, height in enumerate(heights):
        own, got, last = refs[3 * i : 3 * i + 3]
        for m, out in enumerate(refs[3 * len(heights) :]):
            total = own[0, m] + got[0, m].astype(F32) + last[m].astype(F32)
            out[first : first + height, :] = total.astype(out.dtype)
        first += height


def merged(parts, types):
    count, rows = len(types), parts[0][0].shape[3]
    heights = [own.shape[2] for own, _, _ in parts]
    if rows % 128:
        sums = [own[1] + got[1].astype(F32) + last.astype(F32) for own, got, last in parts]
        both = jnp.concatenate(sums, 1)
        return [both[m].astype(dtype) for m, dtype in enumerate(types)]
    in_specs = []
    for height in heights:
        half = pl.BlockSpec((1, count, height, rows), lambda i: (1, 0, 0, 0))
        in_specs += [half, half, pl.BlockSpec((count, height, rows), lambda i: (0, 0, 0))]
    shape = (sum(heights), rows)
    return local_kernel(
        functools.partial(merge_kernel, heights),
        in_specs,
        [pl.BlockSpec(shape, lambda i: (0, 0))] * count,
        [jax.ShapeDtypeStruct(shape, dtype) for dtype in types],
    )(*(value for part in parts for value in part))


def spread_kernel(*refs):
    outs = refs[-4:]
    _, _, y, c = position()
    places = [row * 2 + core for core in (c, 1 - c) for row in (y, 1 - y)]
    for k, piece in enumerate(refs[:-4]):
        for place, out in zip(places, outs):
            out[k] = piece[:, place]


def spread(pieces):
    slots, _, half, order = pieces[0].shape
    shape = (len(pieces), slots, half, order)
    if half % 16:
        _, _, y, c = position()
        both = jnp.stack(pieces)
        places = [row * 2 + core for core in (c, 1 - c) for row in (y, 1 - y)]
        return [pick(both, place, 2) for place in places]
    whole = pl.BlockSpec(pieces[0].shape, lambda i: (0, 0, 0, 0))
    return local_kernel(
        spread_kernel,
        [whole] * len(pieces),
        [pl.BlockSpec(shape, lambda i: (0, 0, 0, 0))] * 4,
        [jax.ShapeDtypeStruct(shape, BF16)] * 4,
    )(*pieces)


def shards(tokens_x, key_grad, left_root, slot_grads, right_root, block_slot):
    n_rep, n_shard = lax.axis_size("rep"), lax.axis_size("shard")
    n_out = n_shard // 4
    x, o, y, c = position()

    def permute(value, target):
        pairs = []
        for r in range(n_rep):
            for t in range(n_shard):
                r2, t2 = target(r, t)
                pairs.append((r * n_shard + t, r2 * n_shard + t2))
        return lax.ppermute(value, AXES, pairs)

    def swap_rep(value):
        return permute(value, lambda r, t: (1 - r, t))

    def swap_row(value):
        return permute(value, lambda r, t: (r, t ^ 2))

    def swap_core(value):
        return permute(value, lambda r, t: (r, t ^ 1))

    def shift_out(value, k):
        return permute(value, lambda r, t: (r, (t // 4 + k) % n_out * 4 + t % 4))

    width = key_grad.shape[1]
    wide = width * WIDE // 16
    thin = width // 2 - wide
    other_tokens = swap_core(tokens_x)

    slots, order, _ = left_root.shape
    half = order // n_shard // 2
    ids = jnp.arange(n_shard * slots, dtype=jnp.int32)
    source_out = (o - ids // slots % n_out + n_out) % n_out
    source_row = jnp.bitwise_xor(y, ids // (slots * n_out) % 2)
    source_core = jnp.bitwise_xor(c, ids // (slots * n_out * 2))
    slot_id = (source_out * 4 + source_row * 2 + source_core) * slots + ids % slots
    slot_id, left_root = lax.optimization_barrier((slot_id, left_root))
    pieces, key = owned_blocks(left_root, slot_grads, right_root, key_grad, n_shard, wide)
    other_key = swap_core(key)
    by_out = [pieces[0]] + [shift_out(pieces[k], k) for k in range(1, n_out)]

    finished = []
    for group in groups_of(n_out):
        kept = partial_rows(
            tokens_x, other_tokens, key, other_key, n_shard, group, wide, thin,
            group[-1] < n_out,
        )
        got_a = swap_rep(kept[0])
        far_a = folded(kept[1], got_a)
        parts = [(kept[1], got_a, swap_row(far_a))]
        if len(kept) > 2:
            got_b = swap_row(kept[2])
            far_b = folded(kept[3], got_b)
            parts.append((kept[3], got_b, swap_rep(far_b)))
        sums = merged(parts, [BF16 if k < n_out else F32 for k in group])
        for k, piece in zip(group, sums):
            finished.append(shift_out(piece, k) if k < n_out else piece)

    own, far_row, far_core, far_both = spread(by_out)
    far_row = swap_row(far_row)
    far_core = swap_core(far_core)
    far_both = permute(far_both, lambda r, t: (r, t ^ 3))
    held = jnp.stack([own, far_row, far_core, far_both])
    held = held.reshape(n_shard * slots, half, order)
    chosen = (block_slot[:, None] == slot_id[None, :]).astype(BF16)
    kept = jnp.einsum("bv,vhj->hbj", chosen, held, preferred_element_type=F32).astype(BF16)
    total = finished[-1]
    for piece in finished[:-1]:
        total = total + piece.astype(F32)
    done = lax.reduce_precision(total, 8, 7)
    far_done = swap_rep(done.astype(BF16)).astype(F32)
    low = jnp.where(x == 0, done, far_done)
    high = jnp.where(x == 0, far_done, done)
    grad_key = jnp.concatenate([low[:wide], high[:wide], low[wide:], high[wide:]], 0).T

    far_kept = swap_rep(kept)
    update = lax.dynamic_slice_in_dim(
        jnp.concatenate([kept, far_kept, kept], 0), x * half, 2 * half, 0
    )
    return (grad_key, update)


def solution(mesh):
    return jax.shard_map(
        shards,
        mesh=mesh,
        in_specs=(
            P(("rep", "shard"), None),
            P(("rep", "shard"), None),
            P("shard", None, None),
            P("shard", None, None),
            P("shard", None, None),
            P(),
        ),
        out_specs=(P("shard", None), P("shard", None, None)),
        check_vma=False,
    )
```
